64 devices in a mesh: dp: 4 (over x, y), fsdp: 16 (over z, core).
Axes of the slice: x: 2, y: 2, z: 8, core: 2. Of those that a mesh axis runs over, the one named last changes fastest.
The devices are a block of a 4x4x8 slice.
Arguments:
- hidden: bfloat16 [64, 1536, 1536], P(('dp', 'fsdp')), parts along dimension 0
- g_attn: bfloat16 [1536], P('fsdp')
- w_query: bfloat16 [1536, 1536], P('fsdp')
- w_key: bfloat16 [1536, 256], P('fsdp')
- w_value: bfloat16 [1536, 256], P('fsdp')
- w_out: bfloat16 [1536, 1536], P('fsdp')
- g_mlp: bfloat16 [1536], P('fsdp')
- w_gate: bfloat16 [1536, 8960], P('fsdp')
- w_up: bfloat16 [1536, 8960], P('fsdp')
- w_down: bfloat16 [8960, 1536], P('fsdp')
- cos_tab: float32 [1536, 64], replicated
- sin_tab: float32 [1536, 64], replicated
Outputs:
- output 1: bfloat16 [64, 1536, 1536], P(('dp', 'fsdp')), parts along dimension 0
- output 2: bfloat16 [64, 1536, 2, 128], P(('dp', 'fsdp')), parts along dimension 0
- output 3: bfloat16 [64, 1536, 2, 128], P(('dp', 'fsdp')), parts along dimension 0
There are 4 independent parts. The reference program is written for one: setup_inputs(seed, part) draws one part's arguments, and reference() takes and returns one part's arrays. A program takes and returns all parts, laid end to end along the dimension named above; an argument that names none is the same for every part.
All inputs are finite; a program needn't handle non-finite values.
Results may differ from the reference program's by a relative error of at most 0.0145732.
Values are sent between devices in bfloat16 or wider.
A program may use at most 768 MiB of HBM per device.

```python
import jax
import jax.numpy as jnp
from jax import lax

BATCH_ROWS = 16
SEQ_LEN = 1536
MODEL_DIM = 1536
NUM_HEADS = 12
KV_HEADS = 2
HEAD_DIM = 128
FFN_DIM = 8960
QUERY_BLOCK = 256
ROPE_BASE = 500000.0
NORM_EPS = 1e-5


def make_weight(rng_key, fan_in, fan_out, factor):
    normal_draw = jax.random.normal(rng_key, (fan_in, fan_out), jnp.float32)
    return (normal_draw * (factor * fan_in ** -0.5)).astype(jnp.bfloat16)


def make_gain(rng_key):
    return jax.random.uniform(rng_key, (MODEL_DIM,), jnp.float32, 0.5, 1.5).astype(jnp.bfloat16)


def rope_tables(rng_key):
    start_pos = jax.random.randint(rng_key, (), 0, 8192)
    inv_freq = 1.0 / (ROPE_BASE ** (jnp.arange(0, HEAD_DIM, 2).astype(jnp.float32) / HEAD_DIM))
    positions = (start_pos + jnp.arange(SEQ_LEN)).astype(jnp.float32)
    angles = positions[:, None] * inv_freq[None, :]
    return jnp.cos(angles), jnp.sin(angles)


def setup_inputs(seed: int = 0, part: int = 0) -> dict:
    sub_keys = jax.random.split(jax.random.key(seed), 11)
    part_key = jax.random.fold_in(sub_keys[0], part)
    q_width = NUM_HEADS * HEAD_DIM
    kv_width = KV_HEADS * HEAD_DIM
    hidden = 0.5 * jax.random.normal(part_key, (BATCH_ROWS, SEQ_LEN, MODEL_DIM), jnp.float32)
    cos_tab, sin_tab = rope_tables(sub_keys[10])
    return {
        "hidden": hidden.astype(jnp.bfloat16),
        "g_attn": make_gain(sub_keys[1]),
        "w_query": make_weight(sub_keys[2], MODEL_DIM, q_width, 2.0),
        "w_key": make_weight(sub_keys[3], MODEL_DIM, kv_width, 1.0),
        "w_value": make_weight(sub_keys[4], MODEL_DIM, kv_width, 1.0),
        "w_out": make_weight(sub_keys[5], q_width, MODEL_DIM, 1.0),
        "g_mlp": make_gain(sub_keys[6]),
        "w_gate": make_weight(sub_keys[7], MODEL_DIM, FFN_DIM, 1.0),
        "w_up": make_weight(sub_keys[8], MODEL_DIM, FFN_DIM, 1.0),
        "w_down": make_weight(sub_keys[9], FFN_DIM, MODEL_DIM, 1.0),
        "cos_tab": cos_tab,
        "sin_tab": sin_tab,
    }


def rms_norm(rows_in, gain_vec):
    upcast = rows_in.astype(jnp.float32)
    scaled = upcast * lax.rsqrt(jnp.mean(upcast * upcast, axis=-1, keepdims=True) + NORM_EPS)
    return (scaled * gain_vec.astype(jnp.float32)).astype(jnp.bfloat16)


def apply_rope(heads_in, cos_tab, sin_tab):
    half_dim = HEAD_DIM // 2
    upcast = heads_in.astype(jnp.float32)
    lo_half = upcast[..., :half_dim]
    hi_half = upcast[..., half_dim:]
    cos_bc = cos_tab[:, None, :]
    sin_bc = sin_tab[:, None, :]
    rotated = jnp.concatenate([lo_half * cos_bc - hi_half * sin_bc, hi_half * cos_bc + lo_half * sin_bc], axis=-1)
    return rotated.astype(jnp.bfloat16)


def reference(hidden, g_attn, w_query, w_key, w_value, w_out, g_mlp, w_gate, w_up, w_down, cos_tab, sin_tab):
    group_size = NUM_HEADS // KV_HEADS
    key_pos = jnp.arange(SEQ_LEN)

    def one_sequence(seq_in):
        normed = rms_norm(seq_in, g_attn)
        query_proj = jnp.dot(normed, w_query, preferred_element_type=jnp.float32).astype(jnp.bfloat16)
        key_proj = jnp.dot(normed, w_key, preferred_element_type=jnp.float32).astype(jnp.bfloat16)
        value_proj = jnp.dot(normed, w_value, preferred_element_type=jnp.float32).astype(jnp.bfloat16)
        query_rot = apply_rope(query_proj.reshape(SEQ_LEN, NUM_HEADS, HEAD_DIM), cos_tab, sin_tab)
        key_rot = apply_rope(key_proj.reshape(SEQ_LEN, KV_HEADS, HEAD_DIM), cos_tab, sin_tab)
        value_heads = value_proj.reshape(SEQ_LEN, KV_HEADS, HEAD_DIM)
        query_grp = query_rot.reshape(SEQ_LEN, KV_HEADS, group_size, HEAD_DIM).astype(jnp.float32)
        key_wide = key_rot.astype(jnp.float32)
        value_wide = value_heads.astype(jnp.float32)

        def one_block(block_idx):
            blk_start = block_idx * QUERY_BLOCK
            query_blk = lax.dynamic_slice_in_dim(query_grp, blk_start, QUERY_BLOCK, axis=0)
            scores = jnp.einsum("qkgd,skd->kgqs", query_blk, key_wide) * HEAD_DIM ** -0.5
            query_pos = blk_start + jnp.arange(QUERY_BLOCK)
            scores = jnp.where(key_pos[None, :] <= query_pos[:, None], scores, -jnp.inf)
            prob_bf16 = jax.nn.softmax(scores, axis=-1).astype(jnp.bfloat16)
            mixed_vals = jnp.einsum("kgqs,skd->qkgd", prob_bf16.astype(jnp.float32), value_wide)
            return mixed_vals.astype(jnp.bfloat16)

        attn_heads = lax.map(one_block, jnp.arange(SEQ_LEN // QUERY_BLOCK))
        attn_flat = attn_heads.reshape(SEQ_LEN, NUM_HEADS * HEAD_DIM)
        attn_proj = jnp.dot(attn_flat, w_out, preferred_element_type=jnp.float32).astype(jnp.bfloat16)
        residual = (seq_in.astype(jnp.float32) + attn_proj.astype(jnp.float32)).astype(jnp.bfloat16)
        normed_mlp = rms_norm(residual, g_mlp)
        gate_proj = jnp.dot(normed_mlp, w_gate, preferred_element_type=jnp.float32).astype(jnp.bfloat16)
        up_proj = jnp.dot(normed_mlp, w_up, preferred_element_type=jnp.float32).astype(jnp.bfloat16)
        act_in = (jax.nn.silu(gate_proj.astype(jnp.float32)) * up_proj.astype(jnp.float32)).astype(jnp.bfloat16)
        mlp_out = jnp.dot(act_in, w_down, preferred_element_type=jnp.float32).astype(jnp.bfloat16)
        out_seq = (residual.astype(jnp.float32) + mlp_out.astype(jnp.float32)).astype(jnp.bfloat16)
        return out_seq, key_rot, value_heads

    out_hidden, k_cache, v_cache = lax.map(one_sequence, hidden)
    return (out_hidden, k_cache, v_cache)
```

```python
import functools
import math

import jax
import jax.numpy as jnp
from jax import lax
from jax.experimental import pallas as pl
from jax.experimental.pallas import tpu as pltpu
from jax.sharding import PartitionSpec as P

EPS = 1e-5
F32 = jnp.float32
BF16 = jnp.bfloat16
MESH = pl.DeviceIdType.MESH
RATE = (1, 1)


def _dot(a, b):
    return lax.dot_general(a, b, (((1,), (0,)), ((), ())), preferred_element_type=F32)


def _dot_t(a, b):
    return lax.dot_general(a, b, (((1,), (1,)), ((), ())), preferred_element_type=F32)


def layer_kernel(cfg, x_hbm, wa_in, wo_in, wg_in, wu_in, wd_in, cos_in, sin_in,
                 out_hbm, k_hbm, v_hbm, ga, go, gg, gu, gd,
                 r, h, xb, wt, wd, ct, st, gains,
                 rz, rp, rsib, sz, sp, ssib, lsem, tsem, dsem, osem):
    n, ny, rows, drows, dim, ffn, heads, kvh, hd = cfg
    seq = x_hbm.shape[0]
    qw = heads * hd
    kw = kvh * hd
    ring = n // 2
    hops = ring - 1
    q_r, q_d = rows // 4, dim // 12
    gu_chunks, gu_tiles, tile = 5, 7, 256
    d_chunks = 3
    gcols = gu_tiles * tile
    dcols = dim // d_chunks
    n_chunk = 1 + gu_chunks + d_chunks

    d = lax.axis_index("dp")
    f = lax.axis_index("fsdp")
    x, y = d // ny, d % ny
    c = f % 2
    par = (x + y) % 2
    xp = (x + 1 - 2 * (x % 2)) * ny + y
    yp = x * ny + (y + 1 - 2 * (y % 2))
    sib = f + 1 - 2 * c
    up = (f + 2) % n
    down = (f + n - 2) % n
    dev_up, dev_dn, dev_sib = (d, up), (d, down), (d, sib)
    dev_x, dev_y = (xp, f), (yp, f)

    barrier = pltpu.get_barrier_semaphore()
    for dev in (dev_up, dev_dn, dev_sib, dev_x, dev_y):
        pl.semaphore_signal(barrier, inc=1, device_id=dev, device_id_type=MESH)
    pl.semaphore_wait(barrier, 5)

    bounce = [
        (wa_in, r.at[pl.ds(0, rows), pl.ds(0, wa_in.shape[1])], ga.at[pl.ds(rows * f, rows), :]),
        (wo_in, r.at[pl.ds(rows, rows), pl.ds(0, dim)], go.at[pl.ds(rows * f, rows), :]),
        (wg_in, r.at[pl.ds(2 * rows, rows), :], gg.at[pl.ds(rows * f, rows), :]),
        (wu_in, r.at[pl.ds(3 * rows, rows), :], gu.at[pl.ds(rows * f, rows), :]),
        (wd_in, r.at[pl.ds(4 * rows, drows), pl.ds(0, dim)], gd.at[pl.ds(drows * f, drows), :]),
    ]
    loads = [pltpu.make_async_copy(s, b, lsem.at[i]) for i, (s, b, _) in enumerate(bounce)]
    puts = [pltpu.make_async_copy(b, t, lsem.at[i]) for i, (_, b, t) in enumerate(bounce)]
    ld_x = pltpu.make_async_copy(x_hbm, xb, lsem.at[5])
    ld_c = pltpu.make_async_copy(cos_in, ct, lsem.at[6])
    ld_s = pltpu.make_async_copy(sin_in, st, lsem.at[7])

    def k_piece(buf, src, cbase, cols, idx):
        def at(f0, q):
            return buf.at[pl.ds(pl.multiple_of(rows * f0 + q_r * q, 8), q_r), pl.ds(cbase, cols)]

        def own_q(q):
            return src.at[pl.ds(pl.multiple_of(q_r * q, 8), q_r), pl.ds(cbase, cols)]

        own = src.at[:, pl.ds(cbase, cols)]
        own_dst = buf.at[pl.ds(pl.multiple_of(rows * f, 8), rows), pl.ds(cbase, cols)]
        seven = buf.at[pl.ds(0, hops * q_r), pl.ds(cbase, cols)]
        half = buf.at[pl.ds(0, ring * rows), pl.ds(cbase, cols)]
        return at, own_q, own, own_dst, seven, half, idx

    def d_piece(jd, part, idx):
        dh = drows // 2

        def col(q):
            return pl.ds(pl.multiple_of(dcols * jd + q_d * q, 128), q_d)

        def at(f0, q):
            return gd.at[pl.ds(pl.multiple_of(drows * f0 + dh * part, 8), dh), col(q)]

        def own_q(q):
            return wd_in.at[pl.ds(dh * part, dh), col(q)]

        full = pl.ds(pl.multiple_of(dcols * jd, 128), dcols)
        own = wd_in.at[pl.ds(dh * part, dh), full]
        own_dst = gd.at[pl.ds(pl.multiple_of(drows * f + dh * part, 8), dh), full]
        seven = gd.at[pl.ds(0, hops * dh), col(0)]
        half = gd.at[pl.ds(0, ring * dh), full]
        return at, own_q, own, own_dst, seven, half, idx

    def pieces_a():
        aw0 = 1152
        return [k_piece(ga, wa_in, 0, aw0, 0), k_piece(ga, wa_in, aw0, wa_in.shape[1] - aw0, 1),
                k_piece(go, wo_in, 0, dim, 2)]

    def pieces_gu(j):
        cb = pl.multiple_of(gcols * j, 128)
        return [k_piece(gg, wg_in, cb, gcols, 3 + 2 * j), k_piece(gu, wu_in, cb, gcols, 4 + 2 * j)]

    def pieces_d(jd):
        return [d_piece(jd, i, 3 + 2 * gu_chunks + 2 * jd + i) for i in range(2)]

    def rdma(src, dst, ss, rs, dev):
        return pltpu.make_async_remote_copy(src_ref=src, dst_ref=dst, send_sem=ss, recv_sem=rs,
                                            device_id=dev, device_id_type=MESH)

    def step_pieces(pieces, s):
        a = s - 1
        zs = [(0, dev_up, dev_x, (f + 2 * n - 2 * a) % n), (1, dev_dn, dev_y, (f + 2 * a) % n)]
        ax = s - 2
        xs = [(0, dev_x, (f + 2 * n - 2 * ax) % n), (1, dev_y, (f + 2 * ax) % n)]

        @pl.when(s == 1)
        def _():
            for at, own_q, own, own_dst, seven, half, i in pieces:
                for k, dev, _, _ in zs:
                    q = 2 * par + k
                    rdma(own_q(q), at(f, q), sz.at[k, i], rz.at[k, i, 0], dev).start()
                rdma(own, own_dst, ssib.at[i], rsib.at[i], dev_sib).start()

        @pl.when((s >= 2) & (s <= hops + 1))
        def _():
            for at, own_q, own, own_dst, seven, half, i in pieces:
                for k, dev, pdev, org in zs:
                    ref = at(org, 2 * par + k)
                    rdma(ref, ref, sz.at[k, i], rz.at[k, i, a - 1], dev).wait_recv()

                    @pl.when(s <= hops)
                    def _():
                        rdma(ref, ref, sz.at[k, i], rz.at[k, i, a], dev).start()

                    rdma(ref, ref, sp.at[k, i], rp.at[k, i, a - 1], pdev).start()
                    rdma(ref, ref, ssib.at[i], rsib.at[i], dev_sib).start()

        @pl.when(s >= 3)
        def _():
            for at, own_q, own, own_dst, seven, half, i in pieces:
                for k, pdev, org in xs:
                    ref = at(org, 2 * (1 - par) + k)
                    rdma(ref, ref, sp.at[k, i], rp.at[k, i, ax - 1], pdev).wait_recv()
                    rdma(ref, ref, ssib.at[i], rsib.at[i], dev_sib).start()

    def step(J, s):
        @pl.when((J >= 1) & (J <= gu_chunks))
        def _():
            step_pieces(pieces_gu(J - 1), s)

        @pl.when((J > gu_chunks) & (J < n_chunk))
        def _():
            step_pieces(pieces_d(J - 1 - gu_chunks), s)

    def pump(t, carry):
        b, k = t // 7, t % 7
        odd = k % 2

        def one(i, c2):
            step((1 - i) * (b - odd) + i * (b - 2), (1 - i) * ((k + 7 * odd) // 2 + 1) + i * (8 + k // 2))
            return c2

        return lax.fori_loop(0, 1 + (1 - odd) * ((6 - k) // 4), one, carry)

    last_pump = 7 * (n_chunk - 1) + 16

    def wait_sib(pieces):
        for at, own_q, own, own_dst, seven, half, i in pieces:
            rdma(half, half, ssib.at[i], rsib.at[i], dev_sib).wait_recv()

    for cp in loads + [ld_x, ld_c, ld_s]:
        cp.start()
    n_start = hops + 2

    def start_step(t, carry):
        step_pieces(pieces_a(), t + 1)

        @pl.when(t == 0)
        def _():
            for cp in loads:
                cp.wait()
            for cp in puts:
                cp.start()

        @pl.when(t >= 7)
        def _():
            pump(t, 0)

        return carry

    lax.fori_loop(0, n_start, start_step, 0)
    for cp in puts + [ld_x, ld_c, ld_s]:
        cp.wait()
    pcs = pieces_a()
    wait_sib(pcs[:2])

    def load_wt(src, col, width, slot, half):
        return pltpu.make_async_copy(src.at[:, pl.ds(col, width)], wt.at[slot, :, pl.ds(half * tile, width)],
                                     tsem.at[slot, half])

    aw = qw + 2 * kw
    gcp = load_wt(ga, aw, 128, 0, 0)
    gcp.start()
    gcp.wait()
    pick = (lax.broadcasted_iota(jnp.int32, (8, 128), 0) == lax.broadcasted_iota(jnp.int32, (8, 128), 1))
    gains[...] = _dot_t(pick.astype(F32).astype(BF16), wt[0, :, 0:128])

    nb = 256

    def norm(row_gain):
        def body(i, cr):
            m = pl.multiple_of(i * nb, nb)
            xv = xb[pl.ds(m, nb), :].astype(F32)
            sc = lax.rsqrt(jnp.mean(xv * xv, axis=-1, keepdims=True) + EPS)
            h[pl.ds(m, nb), :] = ((xv * sc) * gains[row_gain:row_gain + 1, :]).astype(BF16)
            return cr

        lax.fori_loop(0, seq // nb, body, 0)

    load_wt(ga, 0, 512, 0, 0).start()
    norm(0)

    mb, qb = 512, 256
    a_tiles, o_tiles, n_gu, n_d = aw // 512, dim // 512, gu_chunks * gu_tiles, dim // tile
    n_m = seq // mb
    parts = [1, 1, 1, 2, 2, 3]
    starts = [a_tiles + sum(parts[:i]) for i in range(len(parts) + 1)]
    w_o = starts[-1]
    w_g = w_o + o_tiles
    w_d = w_g + n_gu
    n_items = w_d + n_d * n_m
    group = heads // kvh
    scale = hd ** -0.5
    hpt = 512 // hd

    swap = ((lax.broadcasted_iota(jnp.int32, (hd, hd), 0) + hd // 2) % hd
            == lax.broadcasted_iota(jnp.int32, (hd, hd), 1)).astype(F32).astype(BF16)

    def rope(zb, m):
        cv, sv = ct[pl.ds(m, mb), :], st[pl.ds(m, mb), :]
        return (zb.astype(F32) * cv + _dot(zb, swap) * sv).astype(BF16)

    def qkv_tile(t, is_kv):
        slot = t % 2

        @pl.when(t + 1 < a_tiles)
        def _():
            load_wt(ga, pl.multiple_of((t + 1) * 512, 512), 512, 1 - slot, 0).start()

        load_wt(ga, 0, 512, slot, 0).wait()

        def body(i, cr):
            m = pl.multiple_of(i * mb, mb)
            z = _dot(h[pl.ds(m, mb), :], wt[slot]).astype(BF16)
            for j in range(hpt):
                zj = z[:, j * hd:(j + 1) * hd]
                if not (is_kv and j >= kvh):
                    zj = rope(zj, m)
                r[pl.ds(m, mb), pl.ds(pl.multiple_of((t * hpt + j) * hd, hd), hd)] = zj
            return cr

        lax.fori_loop(0, n_m, body, 0)

    st_k = pltpu.make_async_copy(r.at[:, pl.ds(qw, kw)], k_hbm, osem.at[0])
    st_v = pltpu.make_async_copy(r.at[:, pl.ds(qw + kw, kw)], v_hbm, osem.at[1])

    def attend(b, g):
        lo = b * qb
        cnt = heads // parts[b]
        tri = (lax.broadcasted_iota(jnp.int32, (qb, qb), 0) >= lax.broadcasted_iota(jnp.int32, (qb, qb), 1))

        def one_head(i, cr):
            head = g * cnt + i
            kv = head // group
            q = r[lo:lo + qb, pl.ds(pl.multiple_of(head * hd, hd), hd)]
            kcol = pl.ds(pl.multiple_of(qw + kv * hd, hd), hd)
            vcol = pl.ds(pl.multiple_of(qw + kw + kv * hd, hd), hd)
            s2 = jnp.where(tri, _dot_t(q, r[lo:lo + qb, kcol]), -jnp.inf)
            m = jnp.max(s2, axis=-1, keepdims=True)
            if b:
                s1 = _dot_t(q, r[0:lo, kcol])
                m = jnp.maximum(m, jnp.max(s1, axis=-1, keepdims=True))
                e1 = jnp.exp((s1 - m) * scale)
            e2 = jnp.exp((s2 - m) * scale)
            tot = jnp.sum(e2, axis=-1, keepdims=True)
            if b:
                tot = tot + jnp.sum(e1, axis=-1, keepdims=True)
            inv = 1.0 / tot
            o = _dot((e2 * inv).astype(BF16), r[lo:lo + qb, vcol])
            if b:
                o = o + _dot((e1 * inv).astype(BF16), r[0:lo, vcol])
            r[lo:lo + qb, pl.ds(pl.multiple_of(aw + head * hd, hd), hd)] = o.astype(BF16)
            return cr

        lax.fori_loop(0, cnt, one_head, 0)

    def o_tile(t):
        slot = t % 2

        @pl.when(t + 1 < o_tiles)
        def _():
            load_wt(go, pl.multiple_of((t + 1) * 512, 512), 512, 1 - slot, 0).start()

        load_wt(go, 0, 512, slot, 0).wait()
        cols = pl.ds(pl.multiple_of(t * 512, 512), 512)

        def body(i, cr):
            m = pl.multiple_of(i * mb, mb)
            a = _dot(r[pl.ds(m, mb), pl.ds(aw, qw)], wt[slot]).astype(BF16).astype(F32)
            xb[pl.ds(m, mb), cols] = (xb[pl.ds(m, mb), cols].astype(F32) + a).astype(BF16)
            return cr

        lax.fori_loop(0, n_m, body, 0)

    def load_gu(t, slot):
        cb = pl.multiple_of(t * tile, tile)
        return [load_wt(gg, cb, tile, slot, 0), load_wt(gu, cb, tile, slot, 1)]

    def fetch_gu(t):
        @pl.when(t % gu_tiles == 0)
        def _():
            wait_sib(pieces_gu(t // gu_tiles))

        for cp in load_gu(t, t % 2):
            cp.start()

    def gu_tile(t):
        slot = t % 2
        for cp in load_gu(t, slot):
            cp.wait()

        @pl.when(t + 1 < n_gu)
        def _():
            fetch_gu(t + 1)

        def body(i, c2):
            m = pl.multiple_of(i * mb, mb)
            z = _dot(h[pl.ds(m, mb), :], wt[slot])
            g = z[:, :tile].astype(BF16).astype(F32)
            u = z[:, tile:].astype(BF16).astype(F32)
            r[pl.ds(m, mb), pl.ds(pl.multiple_of(t * tile, tile), tile)] = (g / (1.0 + jnp.exp(-g)) * u).astype(BF16)
            return c2

        lax.fori_loop(0, n_m, body, 0)

    dt = dcols // tile

    def load_d(t):
        return pltpu.make_async_copy(gd.at[:, pl.ds(pl.multiple_of(t * tile, tile), tile)], wd.at[t % 2],
                                     dsem.at[t % 2])

    def store_d(t):
        cols = pl.ds(pl.multiple_of(t * tile, tile), tile)
        return pltpu.make_async_copy(xb.at[:, cols], out_hbm.at[:, cols], osem.at[2 + t])

    def d_item(i):
        t, mi = i // n_m, i % n_m

        @pl.when(mi == 0)
        def _():
            @pl.when(t % dt == 0)
            def _():
                wait_sib(pieces_d(t // dt))
                load_d(t).start()

            @pl.when(t % dt != dt - 1)
            def _():
                load_d(t + 1).start()

            load_d(t).wait()

        m = pl.multiple_of(mi * mb, mb)
        mm = _dot(r[pl.ds(m, mb), :], wd[t % 2]).astype(BF16).astype(F32)
        cols = pl.ds(pl.multiple_of(t * tile, tile), tile)
        xb[pl.ds(m, mb), cols] = (xb[pl.ds(m, mb), cols].astype(F32) + mm).astype(BF16)

        @pl.when(mi == n_m - 1)
        def _():
            store_d(t).start()

    def pumps_before(w):
        flat = jnp.minimum(w, w_g)
        up_ = jnp.minimum(jnp.maximum(w - w_g, 0), n_gu)
        rest = jnp.maximum(w - w_d, 0)
        return jnp.minimum(n_start + flat + (up_ * RATE[0]) // RATE[1] + rest, last_pump + 1)

    def item(w, carry):
        lax.fori_loop(pumps_before(w), pumps_before(w + 1), pump, 0)

        @pl.when(w < a_tiles - 1)
        def _():
            qkv_tile(w, False)

        @pl.when(w == a_tiles - 1)
        def _():
            qkv_tile(w, True)
            st_k.start()
            st_v.start()

        for b in range(len(parts)):
            @pl.when((w >= starts[b]) & (w < starts[b + 1]))
            def _(b=b):
                attend(b, w - starts[b])

        @pl.when(w == w_o)
        def _():
            wait_sib(pcs[2:])
            load_wt(go, 0, 512, 0, 0).start()

        @pl.when((w >= w_o) & (w < w_g))
        def _():
            o_tile(w - w_o)

        @pl.when(w == w_g)
        def _():
            st_k.wait()
            st_v.wait()
            fetch_gu(0)
            norm(1)

        @pl.when((w >= w_g) & (w < w_d))
        def _():
            gu_tile(w - w_g)

        @pl.when(w >= w_d)
        def _():
            d_item(w - w_d)

        return carry

    lax.fori_loop(0, n_items, item, 0)
    lax.fori_loop(0, n_d, lambda t, c2: (store_d(t).wait(), c2)[1], 0)

    def drain(pieces):
        for at, own_q, own, own_dst, seven, half, i in pieces:
            for k in range(2):
                rdma(seven, seven, sz.at[k, i], rz.at[k, i, 0], dev_up).wait_send()
                rdma(seven, seven, sp.at[k, i], rp.at[k, i, 0], dev_x).wait_send()
            rdma(half, half, ssib.at[i], rsib.at[i], dev_sib).wait_send()

    drain(pcs)
    lax.fori_loop(0, gu_chunks, lambda j, c2: (drain(pieces_gu(j)), c2)[1], 0)
    lax.fori_loop(0, d_chunks, lambda j, c2: (drain(pieces_d(j)), c2)[1], 0)


def solution(mesh):
    n = mesh.shape["fsdp"]
    ny = math.isqrt(mesh.shape["dp"])
    tok = P(("dp", "fsdp"), None, None)
    cache = P(("dp", "fsdp"), None, None, None)
    row, vec, tab = P("fsdp", None), P("fsdp"), P(None, None)

    def local(hidden, g_attn, w_query, w_key, w_value, w_out, g_mlp, w_gate, w_up, w_down, cos_tab, sin_tab):
        _, seq, dim = hidden.shape
        hd = 2 * cos_tab.shape[1]
        heads, kvh = w_query.shape[1] // hd, w_key.shape[1] // hd
        rows, ffn = w_gate.shape
        drows = w_down.shape[0]
        kw = kvh * hd
        gcol = jnp.pad(jnp.stack([g_attn, g_mlp], axis=1), ((0, 0), (0, 126)))
        wa = jnp.concatenate([w_query, w_key, w_value, gcol], axis=1)
        cos2 = jnp.concatenate([cos_tab, cos_tab], axis=1)
        sin2 = jnp.concatenate([-sin_tab, sin_tab], axis=1)
        cfg = (n, ny, rows, drows, dim, ffn, heads, kvh, hd)
        np_ = 19
        hops = n // 2 - 1
        hbm = pl.BlockSpec(memory_space=pl.ANY)
        sh = jax.ShapeDtypeStruct
        dma = pltpu.SemaphoreType.DMA
        outs = pl.pallas_call(
            functools.partial(layer_kernel, cfg),
            out_shape=[
                sh((seq, dim), BF16), sh((seq, kw), BF16), sh((seq, kw), BF16),
                sh((rows * n, wa.shape[1]), BF16), sh((rows * n, dim), BF16),
                sh((rows * n, ffn), BF16), sh((rows * n, ffn), BF16), sh((drows * n, dim), BF16),
            ],
            in_specs=[hbm] * 8,
            out_specs=[hbm] * 8,
            scratch_shapes=[
                pltpu.VMEM((seq, ffn), BF16), pltpu.VMEM((seq, dim), BF16), pltpu.VMEM((seq, dim), BF16),
                pltpu.VMEM((2, dim, 512), BF16), pltpu.VMEM((2, ffn, 256), BF16),
                pltpu.VMEM((seq, hd), F32), pltpu.VMEM((seq, hd), F32), pltpu.VMEM((8, dim), F32),
                dma((2, np_, hops)), dma((2, np_, hops)), dma((np_,)),
                dma((2, np_)), dma((2, np_)), dma((np_,)),
                dma((8,)), dma((2, 2)), dma((2,)), dma((8,)),
            ],
            compiler_params=pltpu.CompilerParams(collective_id=0, has_side_effects=True,
                                                 vmem_limit_bytes=67043328),
            name="layer",
        )(hidden[0], wa, w_out, w_gate, w_up, w_down, cos2, sin2)
        out, k, v = outs[:3]
        return out[None], k.reshape(1, seq, kvh, hd), v.reshape(1, seq, kvh, hd)

    return jax.shard_map(local, mesh=mesh,
                         in_specs=(tok, vec, row, row, row, row, vec, row, row, row, tab, tab),
                         out_specs=(tok, cache, cache), check_vma=False)
```

```python
import functools
import math

import jax
import jax.numpy as jnp
from jax import lax
from jax.experimental import pallas as pl
from jax.experimental.pallas import tpu as pltpu
from jax.sharding import PartitionSpec as P

EPS = 1e-5
F32 = jnp.float32
BF16 = jnp.bfloat16
MESH = pl.DeviceIdType.MESH
RATE = (1, 1)
STACK = 3
MB = 1536


def _dot(a, b):
    return lax.dot_general(a, b, (((1,), (0,)), ((), ())), preferred_element_type=F32)


def _dot_t(a, b):
    return lax.dot_general(a, b, (((1,), (1,)), ((), ())), preferred_element_type=F32)


def layer_kernel(cfg, x_hbm, wa_in, wo_in, wg_in, wu_in, wd_in, cos_in, sin_in,
                 out_hbm, k_hbm, v_hbm, ga, go, gu, gd,
                 r, h, xb, wt, wd, ct, st, gains,
                 rz, rp, rsib, sz, sp, ssib, lsem, tsem, dsem, osem):
    n, ny, rows, drows, dim, ffn, heads, kvh, hd = cfg
    seq = x_hbm.shape[0]
    qw = heads * hd
    kw = kvh * hd
    ring = n // 2
    hops = ring - 1
    q_r, q_d = rows // 4, dim // 12
    gu_chunks, gu_tiles, tile = 5, 7, 256
    d_chunks = 3
    gcols = gu_tiles * tile
    dcols = dim // d_chunks
    n_chunk = 1 + gu_chunks + d_chunks

    d = lax.axis_index("dp")
    f = lax.axis_index("fsdp")
    x, y = d // ny, d % ny
    c = f % 2
    par = (x + y) % 2
    xp = (x + 1 - 2 * (x % 2)) * ny + y
    yp = x * ny + (y + 1 - 2 * (y % 2))
    sib = f + 1 - 2 * c
    up = (f + 2) % n
    down = (f + n - 2) % n
    dev_up, dev_dn, dev_sib = (d, up), (d, down), (d, sib)
    dev_x, dev_y = (xp, f), (yp, f)

    barrier = pltpu.get_barrier_semaphore()
    for dev in (dev_up, dev_dn, dev_sib, dev_x, dev_y):
        pl.semaphore_signal(barrier, inc=1, device_id=dev, device_id_type=MESH)
    pl.semaphore_wait(barrier, 5)

    bounce = [
        (wa_in, r.at[pl.ds(0, rows), pl.ds(0, wa_in.shape[1])], ga.at[pl.ds(rows * f, rows), :]),
        (wo_in, r.at[pl.ds(rows, rows), pl.ds(0, dim)], go.at[pl.ds(rows * f, rows), :]),
        (wg_in, r.at[pl.ds(2 * rows, rows), :], gu.at[0, pl.ds(rows * f, rows), :]),
        (wu_in, r.at[pl.ds(3 * rows, rows), :], gu.at[1, pl.ds(rows * f, rows), :]),
        (wd_in, r.at[pl.ds(4 * rows, drows), pl.ds(0, dim)], gd.at[pl.ds(drows * f, drows), :]),
    ]
    loads = [pltpu.make_async_copy(s, b, lsem.at[i]) for i, (s, b, _) in enumerate(bounce)]
    puts = [pltpu.make_async_copy(b, t, lsem.at[i]) for i, (_, b, t) in enumerate(bounce)]
    ld_x = pltpu.make_async_copy(x_hbm, xb, lsem.at[5])
    ld_c = pltpu.make_async_copy(cos_in, ct, lsem.at[6])
    ld_s = pltpu.make_async_copy(sin_in, st, lsem.at[7])

    def k_piece(buf, src, cbase, cols, idx):
        def at(f0, q):
            return buf.at[pl.ds(pl.multiple_of(rows * f0 + q_r * q, 8), q_r), pl.ds(cbase, cols)]

        def own_q(q):
            return src.at[pl.ds(pl.multiple_of(q_r * q, 8), q_r), pl.ds(cbase, cols)]

        own = src.at[:, pl.ds(cbase, cols)]
        own_dst = buf.at[pl.ds(pl.multiple_of(rows * f, 8), rows), pl.ds(cbase, cols)]
        seven = buf.at[pl.ds(0, hops * q_r), pl.ds(cbase, cols)]
        half = buf.at[pl.ds(0, ring * rows), pl.ds(cbase, cols)]
        return at, own_q, own, own_dst, seven, half, idx

    def d_piece(jd, idx):
        def col(q):
            return pl.ds(pl.multiple_of(dcols * jd + q_d * q, 128), q_d)

        def at(f0, q):
            return gd.at[pl.ds(pl.multiple_of(drows * f0, 8), drows), col(q)]

        full = pl.ds(pl.multiple_of(dcols * jd, 128), dcols)
        own = gd.at[pl.ds(pl.multiple_of(drows * f, 8), drows), full]
        seven = gd.at[pl.ds(0, hops * drows), col(0)]
        half = gd.at[pl.ds(0, ring * drows), full]
        return at, functools.partial(at, f), own, own, seven, half, idx

    def pieces_a():
        aw0 = 1152
        return [k_piece(ga, wa_in, 0, aw0, 0), k_piece(ga, wa_in, aw0, wa_in.shape[1] - aw0, 1),
                k_piece(go, wo_in, 0, dim, 2)]

    def gu_piece(j, idx):
        cols = pl.ds(pl.multiple_of(gcols * j, 128), gcols)

        def at(f0, q):
            return gu.at[:, pl.ds(pl.multiple_of(rows * f0 + q_r * q, 8), q_r), cols]

        own = gu.at[:, pl.ds(pl.multiple_of(rows * f, 8), rows), cols]
        seven = gu.at[:, pl.ds(0, hops * q_r), cols]
        half = gu.at[:, pl.ds(0, ring * rows), cols]
        return at, functools.partial(at, f), own, own, seven, half, idx

    def pieces_gu(j):
        return [gu_piece(j, 3 + j)]

    def pieces_d(jd):
        return [d_piece(jd, 3 + gu_chunks + jd)]

    def rdma(src, dst, ss, rs, dev):
        return pltpu.make_async_remote_copy(src_ref=src, dst_ref=dst, send_sem=ss, recv_sem=rs,
                                            device_id=dev, device_id_type=MESH)

    def step_pieces(pieces, s):
        a = s - 1
        zs = [(0, dev_up, dev_x, (f + 2 * n - 2 * a) % n), (1, dev_dn, dev_y, (f + 2 * a) % n)]
        ax = s - 2
        xs = [(0, dev_x, (f + 2 * n - 2 * ax) % n), (1, dev_y, (f + 2 * ax) % n)]

        @pl.when(s == 1)
        def _():
            for at, own_q, own, own_dst, seven, half, i in pieces:
                for k, dev, _, _ in zs:
                    q = 2 * par + k
                    rdma(own_q(q), at(f, q), sz.at[k, i], rz.at[k, i, 0], dev).start()
                rdma(own, own_dst, ssib.at[i], rsib.at[i], dev_sib).start()

        @pl.when((s >= 2) & (s <= hops + 1))
        def _():
            for at, own_q, own, own_dst, seven, half, i in pieces:
                for k, dev, pdev, org in zs:
                    ref = at(org, 2 * par + k)
                    rdma(ref, ref, sz.at[k, i], rz.at[k, i, a - 1], dev).wait_recv()

                    @pl.when(s <= hops)
                    def _():
                        rdma(ref, ref, sz.at[k, i], rz.at[k, i, a], dev).start()

                    rdma(ref, ref, sp.at[k, i], rp.at[k, i, a - 1], pdev).start()
                    rdma(ref, ref, ssib.at[i], rsib.at[i], dev_sib).start()

        @pl.when(s >= 3)
        def _():
            for at, own_q, own, own_dst, seven, half, i in pieces:
                for k, pdev, org in xs:
                    ref = at(org, 2 * (1 - par) + k)
                    rdma(ref, ref, sp.at[k, i], rp.at[k, i, ax - 1], pdev).wait_recv()
                    rdma(ref, ref, ssib.at[i], rsib.at[i], dev_sib).start()

    def step(J, s):
        @pl.when((J >= 1) & (J <= gu_chunks))
        def _():
            step_pieces(pieces_gu(J - 1), s)

        @pl.when((J > gu_chunks) & (J < n_chunk))
        def _():
            step_pieces(pieces_d(J - 1 - gu_chunks), s)

    def pump(t, carry):
        lane, i = (t - 7) % 2, (t - 7) // 2
        J, s = 1 + 2 * (i // 7) + lane, i % 7 + 1

        def one(e, c2):
            step(J - 2 * e, s + 7 * e)
            return c2

        return lax.fori_loop(0, 1 + (9 - s) // 7, one, carry)

    last_pump = 7 + (n_chunk - 2) % 2 + 2 * (7 * ((n_chunk - 2) // 2 + 1) + 1)

    def wait_sib(pieces):
        for at, own_q, own, own_dst, seven, half, i in pieces:
            rdma(half, half, ssib.at[i], rsib.at[i], dev_sib).wait_recv()

    for cp in loads + [ld_x, ld_c, ld_s]:
        cp.start()
    n_start = hops + 2

    def start_step(t, carry):
        step_pieces(pieces_a(), t + 1)

        @pl.when(t == 0)
        def _():
            for cp in loads:
                cp.wait()
            for cp in puts:
                cp.start()

        @pl.when(t == 7)
        def _():
            for cp in puts:
                cp.wait()

        @pl.when(t >= 7)
        def _():
            pump(t, 0)

        return carry

    lax.fori_loop(0, n_start, start_step, 0)
    for cp in [ld_x, ld_c, ld_s]:
        cp.wait()
    pcs = pieces_a()
    wait_sib(pcs[:2])

    def load_wt(src, col, width, slot, half):
        return pltpu.make_async_copy(src.at[:, pl.ds(col, width)], wt.at[slot, :, pl.ds(half * tile, width)],
                                     tsem.at[slot, half])

    aw = qw + 2 * kw
    gcp = load_wt(ga, aw, 128, 0, 0)
    gcp.start()
    gcp.wait()
    pick = (lax.broadcasted_iota(jnp.int32, (8, 128), 0) == lax.broadcasted_iota(jnp.int32, (8, 128), 1))
    gains[...] = _dot_t(pick.astype(F32).astype(BF16), wt[0, :, 0:128])

    nb = 256

    def norm(row_gain):
        def body(i, cr):
            m = pl.multiple_of(i * nb, nb)
            xv = xb[pl.ds(m, nb), :].astype(F32)
            sc = lax.rsqrt(jnp.mean(xv * xv, axis=-1, keepdims=True) + EPS)
            h[pl.ds(m, nb), :] = ((xv * sc) * gains[row_gain:row_gain + 1, :]).astype(BF16)
            return cr

        lax.fori_loop(0, seq // nb, body, 0)

    load_wt(ga, 0, 512, 0, 0).start()
    norm(0)

    mb, qb = MB, 256
    a_tiles, o_tiles, n_gu, n_d = aw // 512, dim // 512, gu_chunks * gu_tiles, dim // tile
    n_m = seq // mb
    db = 512
    n_dm = seq // db
    parts = [1, 1, 1, 2, 2, 4]
    starts = [a_tiles + sum(parts[:i]) for i in range(len(parts) + 1)]
    w_o = starts[-1]
    w_g = w_o + o_tiles
    w_d = w_g + n_gu
    n_items = w_d + n_d * n_dm
    group = heads // kvh
    scale = hd ** -0.5
    hpt = 512 // hd

    row_i = lax.broadcasted_iota(jnp.int32, (hd, hd), 0)
    col_i = lax.broadcasted_iota(jnp.int32, (hd, hd), 1)
    swap = ((row_i + hd // 2 == col_i).astype(F32) - (row_i == col_i + hd // 2).astype(F32)).astype(BF16)

    def rope(zb, m):
        cv, sv = ct[pl.ds(m, mb), :], st[pl.ds(m, mb), :]
        return (zb.astype(F32) * cv + _dot(zb, swap) * sv).astype(BF16)

    def qkv_tile(t, is_kv):
        slot = t % 2

        @pl.when(t + 1 < a_tiles)
        def _():
            load_wt(ga, pl.multiple_of((t + 1) * 512, 512), 512, 1 - slot, 0).start()

        load_wt(ga, 0, 512, slot, 0).wait()

        def body(i, cr):
            m = pl.multiple_of(i * mb, mb)
            z = _dot(h[pl.ds(m, mb), :], wt[slot]).astype(BF16)
            for j in range(hpt):
                zj = z[:, j * hd:(j + 1) * hd]
                if not (is_kv and j >= kvh):
                    zj = rope(zj, m)
                head = t * hpt + j
                if is_kv:
                    r[pl.ds(m, mb), pl.ds(pl.multiple_of(head * hd, hd), hd)] = zj
                    continue
                for e in range(mb // qb):
                    col = ((head // group) * (seq // qb) + i * (mb // qb) + e) * hd
                    r[pl.ds(pl.multiple_of((head % group) * qb, qb), qb), pl.ds(pl.multiple_of(col, hd), hd)] = (
                        zj[e * qb:(e + 1) * qb])
            return cr

        lax.fori_loop(0, n_m, body, 0)

    st_k = pltpu.make_async_copy(r.at[:, pl.ds(qw, kw)], k_hbm, osem.at[0])
    st_v = pltpu.make_async_copy(r.at[:, pl.ds(qw + kw, kw)], v_hbm, osem.at[1])

    def attend(b, g):
        lo = b * qb
        n_st = heads // STACK
        cnt = n_st // parts[b]
        per = group // STACK
        sq = STACK * qb
        tri = (lax.broadcasted_iota(jnp.int32, (sq, qb), 0) % qb >= lax.broadcasted_iota(jnp.int32, (sq, qb), 1))

        def heads_at(i, cr):
            unit = g * cnt + i
            kv, part = unit // per, unit % per
            q = r[pl.ds(pl.multiple_of(part * sq, sq), sq), pl.ds(pl.multiple_of((kv * (seq // qb) + b) * hd, hd), hd)]
            kcol = pl.ds(pl.multiple_of(qw + kv * hd, hd), hd)
            vcol = pl.ds(pl.multiple_of(qw + kw + kv * hd, hd), hd)
            s2 = jnp.where(tri, _dot_t(q, r[lo:lo + qb, kcol]), -jnp.inf)
            m = jnp.max(s2, axis=-1, keepdims=True)
            if b:
                s1 = _dot_t(q, r[0:lo, kcol])
                m = jnp.maximum(m, jnp.max(s1, axis=-1, keepdims=True))
            ms = m * scale
            tot = jnp.sum(jnp.exp(s2 * scale - ms), axis=-1, keepdims=True)
            if b:
                tot = tot + jnp.sum(jnp.exp(s1 * scale - ms), axis=-1, keepdims=True)
            lse = ms + jnp.log(tot)
            o = _dot(jnp.exp(s2 * scale - lse).astype(BF16), r[lo:lo + qb, vcol])
            if b:
                o = o + _dot(jnp.exp(s1 * scale - lse).astype(BF16), r[0:lo, vcol])
            o = o.astype(BF16)
            for j in range(STACK):
                col = aw + (kv * group + part * STACK + j) * hd
                r[lo:lo + qb, pl.ds(pl.multiple_of(col, hd), hd)] = o[j * qb:(j + 1) * qb]
            return cr

        lax.fori_loop(0, cnt, heads_at, 0)

    def o_tile(t):
        slot = t % 2

        @pl.when(t + 1 < o_tiles)
        def _():
            load_wt(go, pl.multiple_of((t + 1) * 512, 512), 512, 1 - slot, 0).start()

        load_wt(go, 0, 512, slot, 0).wait()
        cols = pl.ds(pl.multiple_of(t * 512, 512), 512)

        def body(i, cr):
            m = pl.multiple_of(i * mb, mb)
            a = _dot(r[pl.ds(m, mb), pl.ds(aw, qw)], wt[slot]).astype(BF16).astype(F32)
            xb[pl.ds(m, mb), cols] = (xb[pl.ds(m, mb), cols].astype(F32) + a).astype(BF16)
            return cr

        lax.fori_loop(0, n_m, body, 0)

    def load_gu(t, slot):
        cb = pl.multiple_of(t * tile, tile)
        return [load_wt(gu.at[k], cb, tile, slot, k) for k in range(2)]

    def fetch_gu(t):
        @pl.when(t % gu_tiles == 0)
        def _():
            wait_sib(pieces_gu(t // gu_tiles))

        for cp in load_gu(t, (t + 1) % 2):
            cp.start()

    def gu_tile(t):
        slot = (t + 1) % 2
        for cp in load_gu(t, slot):
            cp.wait()

        @pl.when(t + 1 < n_gu)
        def _():
            fetch_gu(t + 1)

        def body(i, c2):
            m = pl.multiple_of(i * mb, mb)
            z = _dot(h[pl.ds(m, mb), :], wt[slot])
            g = z[:, :tile].astype(BF16).astype(F32)
            u = z[:, tile:].astype(BF16).astype(F32)
            r[pl.ds(m, mb), pl.ds(pl.multiple_of(t * tile, tile), tile)] = (g / (1.0 + jnp.exp(-g)) * u).astype(BF16)
            return c2

        lax.fori_loop(0, n_m, body, 0)

    dt = dcols // tile

    def load_d(t):
        return pltpu.make_async_copy(gd.at[:, pl.ds(pl.multiple_of(t * tile, tile), tile)], wd.at[t % 2],
                                     dsem.at[t % 2])

    def store_d(t):
        cols = pl.ds(pl.multiple_of(t * tile, tile), tile)
        return pltpu.make_async_copy(xb.at[:, cols], out_hbm.at[:, cols], osem.at[2 + t])

    def fetch_d(t):
        wait_sib(pieces_d(t // dt))
        load_d(t).start()

    def d_item(i):
        t, mi = i // n_dm, i % n_dm

        @pl.when(mi == 0)
        def _():
            @pl.when(t % dt != dt - 1)
            def _():
                load_d(t + 1).start()

            load_d(t).wait()

        @pl.when((mi == n_dm - 1) & (t % dt == dt - 1) & (t + 1 < n_d))
        def _():
            fetch_d(t + 1)

        m = pl.multiple_of(mi * db, db)
        mm = _dot(r[pl.ds(m, db), :], wd[t % 2]).astype(BF16).astype(F32)
        cols = pl.ds(pl.multiple_of(t * tile, tile), tile)
        xb[pl.ds(m, db), cols] = (xb[pl.ds(m, db), cols].astype(F32) + mm).astype(BF16)

        @pl.when(mi == n_dm - 1)
        def _():
            store_d(t).start()

    def pumps_before(w):
        flat = jnp.minimum(w, w_g)
        up_ = jnp.minimum(jnp.maximum(w - w_g, 0), n_gu)
        rest = jnp.maximum(w - w_d, 0)
        return jnp.minimum(n_start + flat + (up_ * RATE[0]) // RATE[1] + rest, last_pump + 1)

    def item(w, carry):
        lax.fori_loop(pumps_before(w), pumps_before(w + 1), pump, 0)

        @pl.when(w < a_tiles - 1)
        def _():
            qkv_tile(w, False)

        @pl.when(w == a_tiles - 1)
        def _():
            qkv_tile(w, True)
            st_k.start()
            st_v.start()

        for b in range(len(parts)):
            @pl.when((w >= starts[b]) & (w < starts[b + 1]))
            def _(b=b):
                attend(b, w - starts[b])

        @pl.when(w == w_o - 1)
        def _():
            wait_sib(pcs[2:])
            load_wt(go, 0, 512, 0, 0).start()

        @pl.when(w == w_g - 1)
        def _():
            fetch_gu(0)

        @pl.when(w == w_d - 1)
        def _():
            fetch_d(0)

        @pl.when((w >= w_o) & (w < w_g))
        def _():
            o_tile(w - w_o)

        @pl.when(w == w_g)
        def _():
            st_k.wait()
            st_v.wait()
            norm(1)

        @pl.when((w >= w_g) & (w < w_d))
        def _():
            gu_tile(w - w_g)

        @pl.when(w >= w_d)
        def _():
            d_item(w - w_d)

        return carry

    lax.fori_loop(0, n_items, item, 0)
    lax.fori_loop(0, n_d, lambda t, c2: (store_d(t).wait(), c2)[1], 0)

    def drain(pieces):
        for at, own_q, own, own_dst, seven, half, i in pieces:
            for k in range(2):
                rdma(seven, seven, sz.at[k, i], rz.at[k, i, 0], dev_up).wait_send()
                rdma(seven, seven, sp.at[k, i], rp.at[k, i, 0], dev_x).wait_send()
            rdma(half, half, ssib.at[i], rsib.at[i], dev_sib).wait_send()

    drain(pcs)
    lax.fori_loop(0, gu_chunks, lambda j, c2: (drain(pieces_gu(j)), c2)[1], 0)
    lax.fori_loop(0, d_chunks, lambda j, c2: (drain(pieces_d(j)), c2)[1], 0)


def solution(mesh):
    n = mesh.shape["fsdp"]
    ny = math.isqrt(mesh.shape["dp"])
    tok = P(("dp", "fsdp"), None, None)
    cache = P(("dp", "fsdp"), None, None, None)
    row, vec, tab = P("fsdp", None), P("fsdp"), P(None, None)

    def local(hidden, g_attn, w_query, w_key, w_value, w_out, g_mlp, w_gate, w_up, w_down, cos_tab, sin_tab):
        _, seq, dim = hidden.shape
        hd = 2 * cos_tab.shape[1]
        heads, kvh = w_query.shape[1] // hd, w_key.shape[1] // hd
        rows, ffn = w_gate.shape
        drows = w_down.shape[0]
        kw = kvh * hd
        gcol = jnp.pad(jnp.stack([g_attn, g_mlp], axis=1), ((0, 0), (0, 126)))
        wa = jnp.concatenate([w_query, w_key, w_value, gcol], axis=1)
        cos2 = jnp.concatenate([cos_tab, cos_tab], axis=1)
        sin2 = jnp.concatenate([sin_tab, sin_tab], axis=1)
        cfg = (n, ny, rows, drows, dim, ffn, heads, kvh, hd)
        np_ = 11
        hops = n // 2 - 1
        hbm = pl.BlockSpec(memory_space=pl.ANY)
        sh = jax.ShapeDtypeStruct
        dma = pltpu.SemaphoreType.DMA
        outs = pl.pallas_call(
            functools.partial(layer_kernel, cfg),
            out_shape=[
                sh((seq, dim), BF16), sh((seq, kw), BF16), sh((seq, kw), BF16),
                sh((rows * n, wa.shape[1]), BF16), sh((rows * n, dim), BF16),
                sh((2, rows * n, ffn), BF16), sh((drows * n, dim), BF16),
            ],
            in_specs=[hbm] * 8,
            out_specs=[hbm] * 7,
            scratch_shapes=[
                pltpu.VMEM((seq, ffn), BF16), pltpu.VMEM((seq, dim), BF16), pltpu.VMEM((seq, dim), BF16),
                pltpu.VMEM((2, dim, 512), BF16), pltpu.VMEM((2, ffn, 256), BF16),
                pltpu.VMEM((seq, hd), F32), pltpu.VMEM((seq, hd), F32), pltpu.VMEM((8, dim), F32),
                dma((2, np_, hops)), dma((2, np_, hops)), dma((np_,)),
                dma((2, np_)), dma((2, np_)), dma((np_,)),
                dma((8,)), dma((2, 2)), dma((2,)), dma((8,)),
            ],
            compiler_params=pltpu.CompilerParams(collective_id=0, has_side_effects=True,
                                                 vmem_limit_bytes=67043328),
            name="layer",
        )(hidden[0], wa, w_out, w_gate, w_up, w_down, cos2, sin2)
        out, k, v = outs[:3]
        return out[None], k.reshape(1, seq, kvh, hd), v.reshape(1, seq, kvh, hd)

    return jax.shard_map(local, mesh=mesh,
                         in_specs=(tok, vec, row, row, row, row, vec, row, row, row, tab, tab),
                         out_specs=(tok, cache, cache), check_vma=False)
```
